64 devices in a mesh: dp: 4 (over x, y), sp: 16 (over z, core).
Axes of the slice: x: 2, y: 2, z: 8, core: 2. Of those that a mesh axis runs over, the one named last changes fastest.
The devices are a block of a 4x4x8 slice.
Arguments:
- x_in: bfloat16 [32768, 4096], P(('dp', 'sp')), parts along dimension 0
- w_in: bfloat16 [4096, 16768], replicated
- a_neg: float32 [128], replicated
- dt_bias: float32 [128], replicated
- d_skip: float32 [128], replicated
- w_out: bfloat16 [8192, 4096], replicated
Outputs:
- output: bfloat16 [32768, 4096], P(('dp', 'sp')), parts along dimension 0
There are 4 independent parts. The reference program is written for one: setup_inputs(seed, part) draws one part's arguments, and reference() takes and returns one part's arrays. A program takes and returns all parts, laid end to end along the dimension named above; an argument that names none is the same for every part.
All inputs are finite; a program needn't handle non-finite values.
Results may differ from the reference program's by a relative error of at most 0.00322704.
Values are sent between devices in bfloat16 or wider.
A program may use at most 768 MiB of HBM per device.

```python
import jax
import jax.numpy as jnp
from jax import lax

D_MODEL = 4096
HEADS = 128
HEAD_DIM = 64
STATE_DIM = 128
TOKENS_DEV = 512
SEQ_LEN = 8192
SEG_LEN = 128

INNER_DIM = HEADS * HEAD_DIM
PROJ_DIM = 2 * INNER_DIM + 2 * STATE_DIM + HEADS


def setup_inputs(seed: int = 0, part: int = 0) -> dict:
    root_key = jax.random.key(seed)
    k_x, k_win, k_a, k_bias, k_skip, k_wout = jax.random.split(root_key, 6)
    x_in = jax.random.normal(jax.random.fold_in(k_x, part), (SEQ_LEN, D_MODEL), jnp.float32)
    col_scale = jnp.concatenate([
        jnp.full((2 * INNER_DIM,), 1.0, jnp.float32),
        jnp.full((2 * STATE_DIM,), (STATE_DIM * TOKENS_DEV) ** -0.25, jnp.float32),
        jnp.full((HEADS,), 0.5, jnp.float32),
    ]) * D_MODEL ** -0.5
    w_in = jax.random.normal(k_win, (D_MODEL, PROJ_DIM), jnp.float32) * col_scale
    a_neg = -jax.random.uniform(k_a, (HEADS,), jnp.float32, 0.15, 1.2) / TOKENS_DEV
    dt_bias = jax.random.uniform(k_bias, (HEADS,), jnp.float32, -1.0, 1.0)
    d_skip = jax.random.uniform(k_skip, (HEADS,), jnp.float32, 0.5, 1.5)
    w_out = jax.random.normal(k_wout, (INNER_DIM, D_MODEL), jnp.float32) * INNER_DIM ** -0.5
    return {"x_in": x_in.astype(jnp.bfloat16), "w_in": w_in.astype(jnp.bfloat16), "a_neg": a_neg,
            "dt_bias": dt_bias, "d_skip": d_skip, "w_out": w_out.astype(jnp.bfloat16)}


def reference(x_in, w_in, a_neg, dt_bias, d_skip, w_out):
    causal = jnp.arange(SEG_LEN)[:, None] >= jnp.arange(SEG_LEN)[None, :]
    mask_three = causal[:, :, None]

    def seg_step(h_prev, x_seg):
        projected = jnp.dot(x_seg, w_in, preferred_element_type=jnp.float32).astype(jnp.bfloat16)
        z_gate = projected[:, :INNER_DIM].astype(jnp.float32)
        x_heads = projected[:, INNER_DIM:2 * INNER_DIM].astype(jnp.float32).reshape(SEG_LEN, HEADS, HEAD_DIM)
        b_mat = projected[:, 2 * INNER_DIM:2 * INNER_DIM + STATE_DIM]
        c_mat = projected[:, 2 * INNER_DIM + STATE_DIM:2 * INNER_DIM + 2 * STATE_DIM]
        dt_vals = jax.nn.softplus(projected[:, 2 * INNER_DIM + 2 * STATE_DIM:].astype(jnp.float32) + dt_bias)
        log_cum = jnp.cumsum(dt_vals * a_neg, axis=0)
        scores = jnp.dot(c_mat, b_mat.T, preferred_element_type=jnp.float32)
        decay_mat = jnp.where(mask_three, jnp.exp(jnp.where(mask_three, log_cum[:, None, :] - log_cum[None, :, :], 0.0)), 0.0)
        g_mat = (scores[:, :, None] * decay_mat * dt_vals[None, :, :]).astype(jnp.bfloat16)
        y_intra = jnp.einsum("tsh,shp->thp", g_mat.astype(jnp.float32), x_heads)
        x_weighted = (x_heads * (jnp.exp(log_cum[-1] - log_cum) * dt_vals)[:, :, None]).astype(jnp.bfloat16)
        s_seg = jnp.einsum("shp,sn->hpn", x_weighted.astype(jnp.float32), b_mat.astype(jnp.float32))
        h_cast = h_prev.astype(jnp.bfloat16).astype(jnp.float32)
        y_state = jnp.einsum("tn,hpn->thp", c_mat.astype(jnp.float32), h_cast) * jnp.exp(log_cum)[:, :, None]
        y_all = y_intra + y_state + d_skip[None, :, None] * x_heads
        h_next = jnp.exp(log_cum[-1])[:, None, None] * h_prev + s_seg
        gated = (y_all.reshape(SEG_LEN, INNER_DIM) * jax.nn.silu(z_gate)).astype(jnp.bfloat16)
        y_seg = (x_seg.astype(jnp.float32) + jnp.dot(gated, w_out, preferred_element_type=jnp.float32)).astype(jnp.bfloat16)
        return h_next, y_seg

    h_zero = jnp.zeros((HEADS, HEAD_DIM, STATE_DIM), jnp.float32)
    h_last, y_segs = lax.scan(seg_step, h_zero, x_in.reshape(SEQ_LEN // SEG_LEN, SEG_LEN, D_MODEL))
    return y_segs.reshape(SEQ_LEN, D_MODEL)
```

```python
import functools

import jax
import jax.numpy as jnp
from jax import lax
from jax.experimental import pallas as pl
from jax.experimental.pallas import tpu as pltpu
from jax.sharding import PartitionSpec as P

SEG_LEN = 128
LANES = 128
CHUNK = 512
MASKED = -1e30


def mixer_kernel(seq_devs, x_hbm, w_in, a_neg, dt_bias, d_skip, w_out, out_hbm,
                 x_buf, win_buf, wout_buf, xs_buf, z_buf, acc, s_buf, h_buf, gated_a, gated_b,
                 c_buf, bt_buf, cb_buf, log_buf, q_buf, w1_buf, row_buf,
                 x_sem, win_sem, wout_sem, out_sem, send_sem, recv_sem):
    f32, bf16 = jnp.float32, jnp.bfloat16
    tokens, d_model = x_buf.shape
    inner = xs_buf.shape[1]
    heads = a_neg.shape[1]
    head_dim = inner // heads
    state = c_buf.shape[1]
    chunks = inner // CHUNK
    segs = tokens // SEG_LEN
    heads_chunk = CHUNK // head_dim
    small = 2 * state + heads
    n_tile = min(CHUNK, d_model)
    me = lax.axis_index("sp")
    right = lax.rem(me + 1, seq_devs)
    left = lax.rem(me + seq_devs - 1, seq_devs)
    delay = 4 * (me // 2) + lax.rem(me, 2)

    barrier = pltpu.get_barrier_semaphore()
    for peer in (left, right):
        pl.semaphore_signal(barrier, inc=1, device_id={"sp": peer}, device_id_type=pl.DeviceIdType.MESH)

    def small_copy():
        return pltpu.make_async_copy(w_in.at[:, pl.ds(2 * inner, small)], win_buf.at[0, :, pl.ds(0, small)], win_sem.at[0])

    def win_copy(step):
        column = jnp.where(step <= chunks, inner + CHUNK * (step - 1), CHUNK * (step - 1 - chunks))
        column = pl.multiple_of(column, CHUNK)
        slot = lax.rem(step, 2)
        return pltpu.make_async_copy(w_in.at[:, pl.ds(column, CHUNK)], win_buf.at[slot], win_sem.at[slot])

    def wout_copy(chunk):
        slot = lax.rem(chunk, 2)
        row = pl.multiple_of(CHUNK * chunk, CHUNK)
        return pltpu.make_async_copy(w_out.at[pl.ds(row, CHUNK), :], wout_buf.at[slot], wout_sem.at[slot])

    def state_copy(chunk):
        return pltpu.make_async_remote_copy(
            src_ref=s_buf.at[chunk], dst_ref=h_buf.at[chunk], send_sem=send_sem.at[chunk], recv_sem=recv_sem.at[chunk],
            device_id={"sp": right}, device_id_type=pl.DeviceIdType.MESH)

    x_copy = pltpu.make_async_copy(x_hbm, x_buf, x_sem)
    x_copy.start()
    small_copy().start()
    win_copy(jnp.int32(1)).start()

    @pl.when(me == 0)
    def _():
        def clear(chunk, carry):
            h_buf[chunk] = jnp.zeros(h_buf.shape[1:], f32)
            return carry
        lax.fori_loop(0, chunks, clear, 0)

    x_copy.wait()
    small_copy().wait()

    proj = jnp.dot(x_buf[...], win_buf[0, :, :small], preferred_element_type=f32).astype(bf16)
    c_buf[...] = proj[:, state:2 * state]
    bt_buf[...] = proj[:, :state].astype(f32).T.astype(bf16)
    dt = jax.nn.softplus(proj[:, 2 * state:].astype(f32) + dt_bias[...])
    logs = dt * a_neg[...]
    log_dt = jnp.log(dt)
    row_i = lax.broadcasted_iota(jnp.int32, (SEG_LEN, SEG_LEN), 0)
    col_i = lax.broadcasted_iota(jnp.int32, (SEG_LEN, SEG_LEN), 1)
    tri = jnp.where(row_i >= col_i, 1.0, 0.0).astype(f32)
    total = jnp.zeros((1, heads), f32)
    for seg in range(segs):
        rows = slice(SEG_LEN * seg, SEG_LEN * (seg + 1))
        cum = jnp.dot(tri, logs[rows], preferred_element_type=f32, precision=lax.Precision.HIGHEST)
        last = cum[SEG_LEN - 1:]
        log_buf[rows, :] = cum
        q_buf[:, rows] = (cum - log_dt[rows]).T
        w1_buf[rows, :] = jnp.exp(last - cum) * dt[rows]
        row_buf[seg:seg + 1, :] = jnp.exp(last)
        total = total + last
        cb_buf[rows, :] = jnp.dot(c_buf[rows, :], bt_buf[:, rows], preferred_element_type=f32)
    row_buf[segs:segs + 1, :] = jnp.exp(total)
    row_buf[segs + 1:segs + 2, :] = d_skip[...]
    row_buf[segs + 2:8, :] = jnp.zeros((8 - segs - 2, heads), f32)

    def low_half(rows):
        return lax.broadcasted_iota(jnp.int32, (rows, LANES), 1) < head_dim

    def chunk_heads(values, chunk):
        return pltpu.roll(values, lax.rem(heads - heads_chunk * chunk, heads), 1)

    def spread(rolled, pair):
        rows = rolled.shape[0]
        one = jnp.broadcast_to(rolled[:, 2 * pair:2 * pair + 1], (rows, LANES))
        two = jnp.broadcast_to(rolled[:, 2 * pair + 1:2 * pair + 2], (rows, LANES))
        return jnp.where(low_half(rows), one, two)

    def spread_rows(chunk):
        rolled = chunk_heads(row_buf[...], chunk)
        return jnp.concatenate([spread(rolled, pair) for pair in range(heads_chunk // 2)], axis=1)

    def columns_of(chunk):
        return pl.ds(pl.multiple_of(CHUNK * chunk, CHUNK), CHUNK)

    def seg_state(chunk, seg):
        rows = slice(SEG_LEN * seg, SEG_LEN * (seg + 1))
        rolled = chunk_heads(w1_buf[rows, :], chunk)
        factor = jnp.concatenate([spread(rolled, pair) for pair in range(heads_chunk // 2)], axis=1)
        weighted = (xs_buf[rows, columns_of(chunk)].astype(f32) * factor).astype(bf16)
        return jnp.dot(bt_buf[:, rows], weighted, preferred_element_type=f32)

    def block_state(chunk):
        decay = spread_rows(chunk)
        total_state = seg_state(chunk, 0)
        for seg in range(1, segs):
            total_state = decay[seg:seg + 1] * total_state + seg_state(chunk, seg)
        s_buf[chunk] = total_state

    def relay(step):
        chunk = step - 3 - delay

        @pl.when((chunk >= 0) & (chunk < chunks))
        def _():
            @pl.when(me > 0)
            def _():
                state_copy(chunk).wait_recv()

            @pl.when(me < seq_devs - 1)
            def _():
                decay = spread_rows(chunk)[segs:segs + 1]
                s_buf[chunk] = decay * h_buf[chunk] + s_buf[chunk]

    def forward(step):
        chunk = step - 3 - delay

        @pl.when((chunk >= 0) & (chunk < chunks) & (me < seq_devs - 1))
        def _():
            state_copy(chunk).start()

    def project(step, target, chunk):
        slot = lax.rem(step, 2)
        target[:, columns_of(chunk)] = jnp.dot(
            x_buf[...], win_buf[slot], preferred_element_type=f32).astype(bf16)

    def ssd(chunk, gated):
        columns = columns_of(chunk)
        table = spread_rows(chunk)
        state_now = h_buf[chunk]
        causal = row_i >= col_i
        low = low_half(SEG_LEN)
        for seg in range(segs):
            rows = slice(SEG_LEN * seg, SEG_LEN * (seg + 1))
            y_state = jnp.dot(c_buf[rows, :], state_now.astype(bf16), preferred_element_type=f32)
            rolled = chunk_heads(log_buf[rows, :], chunk)
            q_rows = q_buf[pl.ds(pl.multiple_of(heads_chunk * chunk, heads_chunk), heads_chunk), rows]
            x_seg = xs_buf[rows, columns]
            z_seg = z_buf[rows, columns]
            scores = cb_buf[rows, :]
            for pair in range(heads_chunk // 2):
                lanes = slice(LANES * pair, LANES * (pair + 1))
                logs_pair, mats = [], []
                for head in (2 * pair, 2 * pair + 1):
                    log_t = jnp.broadcast_to(rolled[:, head:head + 1], (SEG_LEN, SEG_LEN))
                    expo = jnp.where(causal, log_t - q_rows[head:head + 1, :], MASKED)
                    mats.append((scores * jnp.exp(expo)).astype(bf16))
                    logs_pair.append(log_t)
                x_pair = x_seg[:, lanes]
                nil = jnp.zeros_like(x_pair)
                rhs = jnp.concatenate([jnp.where(low, x_pair, nil), jnp.where(low, nil, x_pair)], axis=0)
                y_pair = jnp.dot(jnp.concatenate(mats, axis=1), rhs, preferred_element_type=f32)
                y_pair = y_pair + y_state[:, lanes] * jnp.exp(jnp.where(low, logs_pair[0], logs_pair[1]))
                y_pair = y_pair + table[segs + 1:segs + 2, lanes] * x_pair.astype(f32)
                z_pair = z_seg[:, lanes].astype(f32)
                gated[rows, lanes] = (y_pair * (z_pair / (1.0 + jnp.exp(-z_pair)))).astype(bf16)
            if seg < segs - 1:
                state_now = table[seg:seg + 1] * state_now + seg_state(chunk, seg)

    def accumulate(chunk, gated):
        slot = lax.rem(chunk, 2)
        acc[...] += jnp.dot(gated[...], wout_buf[slot], preferred_element_type=f32)

    win_copy(jnp.int32(1)).wait()
    win_copy(jnp.int32(2)).start()
    project(jnp.int32(1), xs_buf, jnp.int32(0))
    pl.semaphore_wait(barrier, 2)

    def xs_step(step, carry):
        relay(step)
        win_copy(step).wait()
        win_copy(step + 1).start()
        forward(step)
        block_state(step - 2)
        project(step, xs_buf, step - 1)
        return carry

    lax.fori_loop(2, chunks + 1, xs_step, 0)
    block_state(jnp.int32(chunks - 1))
    wout_copy(jnp.int32(0)).start()
    wout_copy(jnp.int32(1)).start()

    def z_step(step, carry):
        relay(step)
        win_copy(step).wait()

        @pl.when(step < 2 * chunks)
        def _():
            win_copy(step + 1).start()

        forward(step)
        chunk = step - 1 - chunks
        cleared = d_model // chunks
        acc[:, pl.ds(pl.multiple_of(cleared * chunk, cleared), cleared)] = jnp.zeros((tokens, cleared), f32)
        project(step, z_buf, chunk)
        return carry

    lax.fori_loop(chunks + 1, 2 * chunks + 1, z_step, 0)

    def mix(chunk, gated):
        step = 2 * chunks + 1 + chunk
        relay(step)
        forward(step)
        ssd(chunk, gated)

    def add_product(chunk, gated):
        wout_copy(chunk).wait()
        accumulate(chunk, gated)

        @pl.when(chunk + 2 < chunks)
        def _():
            wout_copy(chunk + 2).start()

    mix(jnp.int32(0), gated_a)

    def out_step(pair, carry):
        mix(2 * pair + 1, gated_b)
        add_product(2 * pair, gated_a)
        mix(2 * pair + 2, gated_a)
        add_product(2 * pair + 1, gated_b)
        return carry

    lax.fori_loop(0, chunks // 2 - 1, out_step, 0)
    mix(jnp.int32(chunks - 1), gated_b)
    add_product(jnp.int32(chunks - 2), gated_a)
    final = jnp.int32(chunks - 1)
    wout_copy(final).wait()

    def out_copy(tile):
        cols = pl.ds(n_tile * tile, n_tile)
        return pltpu.make_async_copy(x_buf.at[:, cols], out_hbm.at[:, cols], out_sem.at[tile])

    for tile in range(d_model // n_tile):
        cols = slice(n_tile * tile, n_tile * (tile + 1))
        product = jnp.dot(gated_b[...], wout_buf[(chunks - 1) % 2, :, cols], preferred_element_type=f32)
        x_buf[:, cols] = (x_buf[:, cols].astype(f32) + (acc[:, cols] + product)).astype(bf16)
        out_copy(tile).start()
    for tile in range(d_model // n_tile):
        out_copy(tile).wait()

    @pl.when(me < seq_devs - 1)
    def _():
        def drain(chunk, carry):
            state_copy(chunk).wait_send()
            return carry
        lax.fori_loop(0, chunks, drain, 0)


def solution(mesh):
    seq_devs = mesh.shape["sp"]
    row_spec = P(("dp", "sp"), None)

    def local_mixer(x_loc, w_in, a_neg, dt_bias, d_skip, w_out):
        f32, bf16 = jnp.float32, jnp.bfloat16
        tokens, d_model = x_loc.shape
        inner = w_out.shape[0]
        heads = a_neg.shape[0]
        state = (w_in.shape[1] - 2 * inner - heads) // 2
        chunks = inner // CHUNK
        any_spec = pl.BlockSpec(memory_space=pl.ANY)
        vmem_spec = pl.BlockSpec(memory_space=pltpu.VMEM)
        return pl.pallas_call(
            functools.partial(mixer_kernel, seq_devs),
            out_shape=jax.ShapeDtypeStruct((tokens, d_model), bf16),
            in_specs=[any_spec, any_spec, vmem_spec, vmem_spec, vmem_spec, any_spec],
            out_specs=any_spec,
            scratch_shapes=[
                pltpu.VMEM((tokens, d_model), bf16),
                pltpu.VMEM((2, d_model, CHUNK), bf16),
                pltpu.VMEM((2, CHUNK, d_model), bf16),
                pltpu.VMEM((tokens, inner), bf16),
                pltpu.VMEM((tokens, inner), bf16),
                pltpu.VMEM((tokens, d_model), f32),
                pltpu.VMEM((chunks, state, CHUNK), f32),
                pltpu.VMEM((chunks, state, CHUNK), f32),
                pltpu.VMEM((tokens, CHUNK), bf16),
                pltpu.VMEM((tokens, CHUNK), bf16),
                pltpu.VMEM((tokens, state), bf16),
                pltpu.VMEM((state, tokens), bf16),
                pltpu.VMEM((tokens, SEG_LEN), f32),
                pltpu.VMEM((tokens, heads), f32),
                pltpu.VMEM((heads, tokens), f32),
                pltpu.VMEM((tokens, heads), f32),
                pltpu.VMEM((8, heads), f32),
                pltpu.SemaphoreType.DMA,
                pltpu.SemaphoreType.DMA((2,)),
                pltpu.SemaphoreType.DMA((2,)),
                pltpu.SemaphoreType.DMA((max(1, d_model // CHUNK),)),
                pltpu.SemaphoreType.DMA((chunks,)),
                pltpu.SemaphoreType.DMA((chunks,)),
            ],
            compiler_params=pltpu.CompilerParams(
                collective_id=0, has_side_effects=True, vmem_limit_bytes=67043328),
        )(x_loc, w_in, a_neg[None], dt_bias[None], d_skip[None], w_out)

    return jax.shard_map(local_mixer, mesh=mesh, in_specs=(row_spec, P(), P(), P(), P(), P()),
                         out_specs=row_spec, check_vma=False)
```

```python
import functools

import jax
import jax.numpy as jnp
from jax import lax
from jax.experimental import pallas as pl
from jax.experimental.pallas import tpu as pltpu
from jax.sharding import PartitionSpec as P

SEG_LEN = 128
LANES = 128
CHUNK = 512
MASKED = -1e30
LOG2E = 1.4426950408889634


def mixer_kernel(seq_devs, x_hbm, w_in, a_neg, dt_bias, d_skip, w_out, out_hbm,
                 x_buf, win_buf, wout_buf, xs_buf, z_buf, acc, s_buf, h_buf, gated_a, gated_b,
                 xw_buf, c_buf, bt_buf, cb_buf, log_buf, q_buf, w1_buf, row_buf, decay_buf,
                 x_sem, win_sem, wout_sem, out_sem, send_sem, recv_sem):
    f32, bf16 = jnp.float32, jnp.bfloat16
    tokens, d_model = x_buf.shape
    inner = xs_buf.shape[1]
    heads = a_neg.shape[1]
    head_dim = inner // heads
    state = c_buf.shape[1]
    chunks = inner // CHUNK
    segs = tokens // SEG_LEN
    heads_chunk = CHUNK // head_dim
    small = 2 * state + heads
    n_tile = min(CHUNK, d_model)
    me = lax.axis_index("sp")
    right = lax.rem(me + 1, seq_devs)
    left = lax.rem(me + seq_devs - 1, seq_devs)
    delay = 4 * (me // 2) + lax.rem(me, 2)

    barrier = pltpu.get_barrier_semaphore()
    for peer in (left, right):
        pl.semaphore_signal(barrier, inc=1, device_id={"sp": peer}, device_id_type=pl.DeviceIdType.MESH)

    def small_copy():
        return pltpu.make_async_copy(w_in.at[:, pl.ds(2 * inner, small)], win_buf.at[0, :, pl.ds(0, small)], win_sem.at[0])

    def win_copy(step):
        column = jnp.where(step <= chunks, inner + CHUNK * (step - 1), CHUNK * (step - 1 - chunks))
        column = pl.multiple_of(column, CHUNK)
        slot = lax.rem(step, 2)
        return pltpu.make_async_copy(w_in.at[:, pl.ds(column, CHUNK)], win_buf.at[slot], win_sem.at[slot])

    def wout_copy(chunk):
        slot = lax.rem(chunk, 2)
        row = pl.multiple_of(CHUNK * chunk, CHUNK)
        return pltpu.make_async_copy(w_out.at[pl.ds(row, CHUNK), :], wout_buf.at[slot], wout_sem.at[slot])

    def state_copy(chunk):
        return pltpu.make_async_remote_copy(
            src_ref=s_buf.at[chunk], dst_ref=h_buf.at[chunk], send_sem=send_sem.at[chunk], recv_sem=recv_sem.at[chunk],
            device_id={"sp": right}, device_id_type=pl.DeviceIdType.MESH)

    x_copy = pltpu.make_async_copy(x_hbm, x_buf, x_sem)
    x_copy.start()
    small_copy().start()
    win_copy(jnp.int32(1)).start()

    @pl.when(me == 0)
    def _():
        def clear(chunk, carry):
            h_buf[chunk] = jnp.zeros(h_buf.shape[1:], f32)
            return carry
        lax.fori_loop(0, chunks, clear, 0)

    x_copy.wait()
    small_copy().wait()

    proj = jnp.dot(x_buf[...], win_buf[0, :, :small], preferred_element_type=f32).astype(bf16)
    win_copy(jnp.int32(1)).wait()
    win_copy(jnp.int32(2)).start()
    xs_buf[:, :CHUNK] = jnp.dot(x_buf[...], win_buf[1], preferred_element_type=f32).astype(bf16)
    c_buf[...] = proj[:, state:2 * state]
    bt_buf[...] = proj[:, :state].astype(f32).T.astype(bf16)
    dt = jax.nn.softplus(proj[:, 2 * state:].astype(f32) + dt_bias[...])
    logs = dt * a_neg[...]
    log_dt = jnp.log(dt) * LOG2E
    row_i = lax.broadcasted_iota(jnp.int32, (SEG_LEN, SEG_LEN), 0)
    col_i = lax.broadcasted_iota(jnp.int32, (SEG_LEN, SEG_LEN), 1)
    tri = jnp.where(row_i >= col_i, 1.0, 0.0).astype(f32)
    total = jnp.zeros((1, heads), f32)
    for seg in range(segs):
        rows = slice(SEG_LEN * seg, SEG_LEN * (seg + 1))
        cum = jnp.dot(tri, logs[rows], preferred_element_type=f32, precision=lax.Precision.HIGHEST)
        last = cum[SEG_LEN - 1:]
        log_buf[rows, :] = cum * LOG2E
        q_buf[:, rows] = (cum * LOG2E - log_dt[rows]).T
        w1_buf[rows, :] = jnp.exp(last - cum) * dt[rows]
        row_buf[seg:seg + 1, :] = jnp.exp(last)
        total = total + last
        cb_buf[rows, :] = jnp.dot(c_buf[rows, :], bt_buf[:, rows], preferred_element_type=f32)
    row_buf[segs:segs + 1, :] = jnp.exp(total)
    row_buf[segs + 1:segs + 2, :] = d_skip[...]
    row_buf[segs + 2:8, :] = jnp.zeros((8 - segs - 2, heads), f32)

    def low_half(rows):
        return lax.broadcasted_iota(jnp.int32, (rows, LANES), 1) < head_dim

    def chunk_heads(values, chunk):
        chunk = jnp.int32(chunk)
        return pltpu.roll(values, lax.rem(heads - heads_chunk * chunk, heads), 1)

    def spread(rolled, pair):
        rows = rolled.shape[0]
        one = jnp.broadcast_to(rolled[:, 2 * pair:2 * pair + 1], (rows, LANES))
        two = jnp.broadcast_to(rolled[:, 2 * pair + 1:2 * pair + 2], (rows, LANES))
        return jnp.where(low_half(rows), one, two)

    def spread_rows(chunk):
        rolled = chunk_heads(row_buf[...], chunk)
        return jnp.concatenate([spread(rolled, pair) for pair in range(heads_chunk // 2)], axis=1)

    def columns_of(chunk):
        if isinstance(chunk, int):
            return slice(CHUNK * chunk, CHUNK * (chunk + 1))
        return pl.ds(pl.multiple_of(CHUNK * chunk, CHUNK), CHUNK)

    def weigh(chunk, seg):
        rows = slice(SEG_LEN * seg, SEG_LEN * (seg + 1))
        rolled = chunk_heads(w1_buf[rows, :], chunk)
        factor = jnp.concatenate([spread(rolled, pair) for pair in range(heads_chunk // 2)], axis=1)
        return (xs_buf[rows, columns_of(chunk)].astype(f32) * factor).astype(bf16)

    def seg_state(weighted, seg):
        return jnp.dot(bt_buf[:, SEG_LEN * seg:SEG_LEN * (seg + 1)], weighted, preferred_element_type=f32)

    def weigh_block(chunk):
        decay_buf[chunk] = spread_rows(chunk)
        for seg in range(segs):
            xw_buf[SEG_LEN * seg:SEG_LEN * (seg + 1), :] = weigh(chunk, seg)

    def block_state(chunk):
        total_state = seg_state(xw_buf[:SEG_LEN, :], 0)
        for seg in range(1, segs):
            total_state = (decay_buf[chunk, seg:seg + 1] * total_state
                           + seg_state(xw_buf[SEG_LEN * seg:SEG_LEN * (seg + 1), :], seg))
        s_buf[chunk] = total_state

    def relay(step):
        chunk = step - 3 - delay

        @pl.when((chunk >= 0) & (chunk < chunks))
        def _():
            @pl.when(me > 0)
            def _():
                state_copy(chunk).wait_recv()

            @pl.when(me < seq_devs - 1)
            def _():
                decay = decay_buf[chunk, segs:segs + 1]
                s_buf[chunk] = decay * h_buf[chunk] + s_buf[chunk]

    def forward(step):
        chunk = step - 3 - delay

        @pl.when((chunk >= 0) & (chunk < chunks) & (me < seq_devs - 1))
        def _():
            state_copy(chunk).start()

    def project(step, target, chunk):
        slot = step % 2 if isinstance(step, int) else lax.rem(step, 2)
        target[:, columns_of(chunk)] = jnp.dot(
            x_buf[...], win_buf[slot], preferred_element_type=f32).astype(bf16)

    def ssd_seg(chunk, seg, state_now, gated):
        columns = columns_of(chunk)
        table = decay_buf.at[chunk]
        low = low_half(SEG_LEN)
        rows = slice(SEG_LEN * seg, SEG_LEN * (seg + 1))
        y_state = jnp.dot(c_buf[rows, :], state_now.astype(bf16), preferred_element_type=f32)
        rolled = chunk_heads(log_buf[rows, :], chunk)
        first_head = heads_chunk * chunk
        if not isinstance(chunk, int):
            first_head = pl.multiple_of(first_head, heads_chunk)
        q_rows = q_buf[pl.ds(first_head, heads_chunk), rows]
        x_seg = xs_buf[rows, columns]
        z_seg = z_buf[rows, columns]
        scores = cb_buf[rows, :]
        causal = row_i >= col_i
        for pair in range(heads_chunk // 2):
            lanes = slice(LANES * pair, LANES * (pair + 1))
            logs_pair, mats = [], []
            for head in (2 * pair, 2 * pair + 1):
                log_t = jnp.broadcast_to(rolled[:, head:head + 1], (SEG_LEN, SEG_LEN))
                expo = jnp.where(causal, log_t - q_rows[head:head + 1, :], MASKED)
                mats.append((scores * jnp.exp2(expo)).astype(bf16))
                logs_pair.append(log_t)
            x_pair = x_seg[:, lanes]
            nil = jnp.zeros_like(x_pair)
            rhs = jnp.concatenate([jnp.where(low, x_pair, nil), jnp.where(low, nil, x_pair)], axis=0)
            y_pair = jnp.dot(jnp.concatenate(mats, axis=1), rhs, preferred_element_type=f32)
            y_pair = y_pair + y_state[:, lanes] * jnp.exp2(jnp.where(low, logs_pair[0], logs_pair[1]))
            y_pair = y_pair + table[segs + 1:segs + 2, lanes] * x_pair.astype(f32)
            z_pair = z_seg[:, lanes].astype(f32)
            gated[rows, lanes] = (y_pair * (z_pair / (1.0 + jnp.exp2(z_pair * -LOG2E)))).astype(bf16)
        if seg < segs - 1:
            state_now = table[seg:seg + 1] * state_now + seg_state(weigh(chunk, seg), seg)
        return state_now

    def mix_and_add(chunk, gated, done, piece_of):
        state_now = h_buf[chunk]
        for seg in range(segs):
            piece_of(seg)
            state_now = ssd_seg(chunk, seg, state_now, gated)

    pl.semaphore_wait(barrier, 2)

    def xs_step(step, carry):
        relay(step)
        win_copy(step).wait()
        win_copy(step + 1).start()
        forward(step)
        weigh_block(step - 2)
        project(step, xs_buf, step - 1)
        block_state(step - 2)
        return carry

    lax.fori_loop(2, chunks + 1, xs_step, 0)

    def z_part(step, chunk):
        cleared = d_model // chunks
        start = cleared * chunk if isinstance(chunk, int) else pl.multiple_of(cleared * chunk, cleared)
        acc[:, pl.ds(start, cleared)] = jnp.zeros((tokens, cleared), f32)
        project(step, z_buf, chunk)

    def z_enter(step):
        step = jnp.int32(step)
        relay(step)
        win_copy(step).wait()
        win_copy(step + 1).start()
        forward(step)

    z_enter(chunks + 1)
    weigh_block(chunks - 1)
    z_part(chunks + 1, 0)
    block_state(chunks - 1)
    wout_copy(jnp.int32(0)).start()

    def z_step(step, carry):
        z_enter(step)
        z_part(step, step - 1 - chunks)
        return carry

    lax.fori_loop(chunks + 2, 2 * chunks, z_step, 0)
    last_z = jnp.int32(2 * chunks)
    relay(last_z)
    win_copy(last_z).wait()
    forward(last_z)
    z_pieces = [z_part] + [lambda step, chunk: None] * (segs - 1)
    mix_and_add(0, gated_a, None, lambda seg: z_pieces[seg](2 * chunks, chunks - 1))

    def out_part(chunk, gated, piece):
        width = d_model // segs
        cols = slice(width * piece, width * (piece + 1))
        slot = chunk % 2 if isinstance(chunk, int) else lax.rem(chunk, 2)
        acc[:, cols] += jnp.dot(gated[...], wout_buf[slot, :, cols], preferred_element_type=f32)

    def out_enter(chunk):
        chunk = jnp.int32(chunk)
        step = 2 * chunks + chunk
        relay(step)
        wout_copy(chunk - 1).wait()
        wout_copy(chunk).start()
        forward(step)

    def out_chunk(chunk, gated, before):
        out_enter(chunk)
        mix_and_add(chunk, gated, before, lambda seg: out_part(chunk - 1, before, seg))

    def out_step(pair, carry):
        out_chunk(2 * pair + 1, gated_b, gated_a)
        out_chunk(2 * pair + 2, gated_a, gated_b)
        return carry

    lax.fori_loop(0, chunks // 2 - 1, out_step, 0)
    out_chunk(chunks - 1, gated_b, gated_a)
    final = jnp.int32(chunks - 1)
    wout_copy(final).wait()

    def out_copy(tile):
        cols = pl.ds(n_tile * tile, n_tile)
        return pltpu.make_async_copy(x_buf.at[:, cols], out_hbm.at[:, cols], out_sem.at[tile])

    for tile in range(d_model // n_tile):
        cols = slice(n_tile * tile, n_tile * (tile + 1))
        product = jnp.dot(gated_b[...], wout_buf[(chunks - 1) % 2, :, cols], preferred_element_type=f32)
        x_buf[:, cols] = (x_buf[:, cols].astype(f32) + (acc[:, cols] + product)).astype(bf16)
        out_copy(tile).start()
    for tile in range(d_model // n_tile):
        out_copy(tile).wait()

    @pl.when(me < seq_devs - 1)
    def _():
        def drain(chunk, carry):
            state_copy(chunk).wait_send()
            return carry
        lax.fori_loop(0, chunks, drain, 0)


def solution(mesh):
    seq_devs = mesh.shape["sp"]
    row_spec = P(("dp", "sp"), None)

    def local_mixer(x_loc, w_in, a_neg, dt_bias, d_skip, w_out):
        f32, bf16 = jnp.float32, jnp.bfloat16
        tokens, d_model = x_loc.shape
        inner = w_out.shape[0]
        heads = a_neg.shape[0]
        state = (w_in.shape[1] - 2 * inner - heads) // 2
        chunks = inner // CHUNK
        any_spec = pl.BlockSpec(memory_space=pl.ANY)
        vmem_spec = pl.BlockSpec(memory_space=pltpu.VMEM)
        return pl.pallas_call(
            functools.partial(mixer_kernel, seq_devs),
            out_shape=jax.ShapeDtypeStruct((tokens, d_model), bf16),
            in_specs=[any_spec, any_spec, vmem_spec, vmem_spec, vmem_spec, any_spec],
            out_specs=any_spec,
            scratch_shapes=[
                pltpu.VMEM((tokens, d_model), bf16),
                pltpu.VMEM((2, d_model, CHUNK), bf16),
                pltpu.VMEM((2, CHUNK, d_model), bf16),
                pltpu.VMEM((tokens, inner), bf16),
                pltpu.VMEM((tokens, inner), bf16),
                pltpu.VMEM((tokens, d_model), f32),
                pltpu.VMEM((chunks, state, CHUNK), f32),
                pltpu.VMEM((chunks, state, CHUNK), f32),
                pltpu.VMEM((tokens, CHUNK), bf16),
                pltpu.VMEM((tokens, CHUNK), bf16),
                pltpu.VMEM((tokens, CHUNK), bf16),
                pltpu.VMEM((tokens, state), bf16),
                pltpu.VMEM((state, tokens), bf16),
                pltpu.VMEM((tokens, SEG_LEN), f32),
                pltpu.VMEM((tokens, heads), f32),
                pltpu.VMEM((heads, tokens), f32),
                pltpu.VMEM((tokens, heads), f32),
                pltpu.VMEM((8, heads), f32),
                pltpu.VMEM((chunks, 8, CHUNK), f32),
                pltpu.SemaphoreType.DMA,
                pltpu.SemaphoreType.DMA((2,)),
                pltpu.SemaphoreType.DMA((2,)),
                pltpu.SemaphoreType.DMA((max(1, d_model // CHUNK),)),
                pltpu.SemaphoreType.DMA((chunks,)),
                pltpu.SemaphoreType.DMA((chunks,)),
            ],
            compiler_params=pltpu.CompilerParams(
                collective_id=0, has_side_effects=True, vmem_limit_bytes=67043328),
        )(x_loc, w_in, a_neg[None], dt_bias[None], d_skip[None], w_out)

    return jax.shard_map(local_mixer, mesh=mesh, in_specs=(row_spec, P(), P(), P(), P(), P()),
                         out_specs=row_spec, check_vma=False)
```

```python
import functools

import jax
import jax.numpy as jnp
from jax import lax
from jax.experimental import pallas as pl
from jax.experimental.pallas import tpu as pltpu
from jax.sharding import PartitionSpec as P

SEG_LEN = 128
LANES = 128
CHUNK = 512
PIECES = 4
MASKED = -1e30
LOG2E = 1.4426950408889634


def mixer_kernel(seq_devs, x_hbm, w_in, a_neg, dt_bias, d_skip, w_out, out_ref,
                 win_buf, wout_buf, xs_buf, z_buf, acc, s_buf, h_buf, gated_a, gated_b,
                 xw_buf, c_buf, bt_buf, cb_buf, log_buf, q_buf, w1_buf, row_buf, decay_buf,
                 x_sem, small_sem, first_sem, win_sem, wout_sem, send_sem, recv_sem):
    f32, bf16 = jnp.float32, jnp.bfloat16
    tokens, d_model = out_ref.shape
    inner = xs_buf.shape[1]
    heads = a_neg.shape[1]
    head_dim = inner // heads
    state = c_buf.shape[1]
    chunks = inner // CHUNK
    segs = tokens // SEG_LEN
    heads_chunk = CHUNK // head_dim
    small = 2 * state + heads
    k_tile = d_model // PIECES
    me = lax.axis_index("sp")
    right = lax.rem(me + 1, seq_devs)
    left = lax.rem(me + seq_devs - 1, seq_devs)
    delay = 4 * (me // 2) + lax.rem(me, 2)

    barrier = pltpu.get_barrier_semaphore()
    for peer in (left, right):
        pl.semaphore_signal(barrier, inc=1, device_id={"sp": peer}, device_id_type=pl.DeviceIdType.MESH)

    def x_copy(piece):
        cols = pl.ds(k_tile * piece, k_tile)
        return pltpu.make_async_copy(x_hbm.at[:, cols], out_ref.at[:, cols], x_sem.at[piece])

    def small_copy(piece):
        rows = pl.ds(k_tile * piece, k_tile)
        return pltpu.make_async_copy(
            w_in.at[rows, pl.ds(2 * inner, small)], win_buf.at[0, rows, pl.ds(0, small)], small_sem.at[piece])

    def first_copy(piece):
        rows = pl.ds(k_tile * piece, k_tile)
        return pltpu.make_async_copy(
            w_in.at[rows, pl.ds(inner, CHUNK)], win_buf.at[1, rows, :], first_sem.at[piece])

    def win_copy(step):
        column = jnp.where(step <= chunks, inner + CHUNK * (step - 1), CHUNK * (step - 1 - chunks))
        column = pl.multiple_of(column, CHUNK)
        slot = lax.rem(step, 2)
        return pltpu.make_async_copy(w_in.at[:, pl.ds(column, CHUNK)], win_buf.at[slot], win_sem.at[slot])

    def wout_copy(chunk):
        slot = lax.rem(chunk, 2)
        row = pl.multiple_of(CHUNK * chunk, CHUNK)
        return pltpu.make_async_copy(w_out.at[pl.ds(row, CHUNK), :], wout_buf.at[slot], wout_sem.at[slot])

    def state_copy(chunk):
        return pltpu.make_async_remote_copy(
            src_ref=s_buf.at[chunk], dst_ref=h_buf.at[chunk], send_sem=send_sem.at[chunk], recv_sem=recv_sem.at[chunk],
            device_id={"sp": right}, device_id_type=pl.DeviceIdType.MESH)

    for piece in range(PIECES):
        x_copy(piece).start()
        small_copy(piece).start()
    for piece in range(PIECES):
        first_copy(piece).start()

    @pl.when(me == 0)
    def _():
        def clear(chunk, carry):
            h_buf[chunk] = jnp.zeros(h_buf.shape[1:], f32)
            return carry
        lax.fori_loop(0, chunks, clear, 0)

    proj = jnp.zeros((tokens, small), f32)
    for piece in range(PIECES):
        x_copy(piece).wait()
        small_copy(piece).wait()
        part = slice(k_tile * piece, k_tile * (piece + 1))
        proj = proj + jnp.dot(out_ref[:, part], win_buf[0, part, :small], preferred_element_type=f32)
    proj = proj.astype(bf16)
    win_copy(jnp.int32(2)).start()
    first = jnp.zeros((tokens, CHUNK), f32)
    for piece in range(PIECES):
        first_copy(piece).wait()
        part = slice(k_tile * piece, k_tile * (piece + 1))
        first = first + jnp.dot(out_ref[:, part], win_buf[1, part, :], preferred_element_type=f32)
    xs_buf[:, :CHUNK] = first.astype(bf16)
    c_buf[...] = proj[:, state:2 * state]
    bt_buf[...] = proj[:, :state].astype(f32).T.astype(bf16)
    dt = jax.nn.softplus(proj[:, 2 * state:].astype(f32) + dt_bias[...])
    logs = dt * a_neg[...]
    log_dt = jnp.log(dt) * LOG2E
    row_i = lax.broadcasted_iota(jnp.int32, (SEG_LEN, SEG_LEN), 0)
    col_i = lax.broadcasted_iota(jnp.int32, (SEG_LEN, SEG_LEN), 1)
    tri = jnp.where(row_i >= col_i, 1.0, 0.0).astype(f32)
    total = jnp.zeros((1, heads), f32)
    for seg in range(segs):
        rows = slice(SEG_LEN * seg, SEG_LEN * (seg + 1))
        cum = jnp.dot(tri, logs[rows], preferred_element_type=f32, precision=lax.Precision.HIGHEST)
        last = cum[SEG_LEN - 1:]
        log_buf[rows, :] = cum * LOG2E
        q_buf[:, rows] = (cum * LOG2E - log_dt[rows]).T
        w1_buf[rows, :] = jnp.exp(last - cum) * dt[rows]
        row_buf[seg:seg + 1, :] = jnp.exp(last)
        total = total + last
        cb_buf[rows, :] = jnp.dot(c_buf[rows, :], bt_buf[:, rows], preferred_element_type=f32)
    row_buf[segs:segs + 1, :] = jnp.exp(total)
    row_buf[segs + 1:segs + 2, :] = d_skip[...]
    row_buf[segs + 2:8, :] = jnp.zeros((8 - segs - 2, heads), f32)

    def low_half(rows):
        return lax.broadcasted_iota(jnp.int32, (rows, LANES), 1) < head_dim

    def chunk_heads(values, chunk):
        chunk = jnp.int32(chunk)
        return pltpu.roll(values, lax.rem(heads - heads_chunk * chunk, heads), 1)

    def spread(rolled, pair):
        rows = rolled.shape[0]
        one = jnp.broadcast_to(rolled[:, 2 * pair:2 * pair + 1], (rows, LANES))
        two = jnp.broadcast_to(rolled[:, 2 * pair + 1:2 * pair + 2], (rows, LANES))
        return jnp.where(low_half(rows), one, two)

    def spread_rows(chunk):
        rolled = chunk_heads(row_buf[...], chunk)
        return jnp.concatenate([spread(rolled, pair) for pair in range(heads_chunk // 2)], axis=1)

    def columns_of(chunk):
        if isinstance(chunk, int):
            return slice(CHUNK * chunk, CHUNK * (chunk + 1))
        return pl.ds(pl.multiple_of(CHUNK * chunk, CHUNK), CHUNK)

    def weigh(chunk, seg):
        rows = slice(SEG_LEN * seg, SEG_LEN * (seg + 1))
        rolled = chunk_heads(w1_buf[rows, :], chunk)
        factor = jnp.concatenate([spread(rolled, pair) for pair in range(heads_chunk // 2)], axis=1)
        return (xs_buf[rows, columns_of(chunk)].astype(f32) * factor).astype(bf16)

    def seg_state(weighted, seg):
        return jnp.dot(bt_buf[:, SEG_LEN * seg:SEG_LEN * (seg + 1)], weighted, preferred_element_type=f32)

    def weigh_block(chunk):
        decay_buf[chunk] = spread_rows(chunk)
        for seg in range(segs):
            xw_buf[SEG_LEN * seg:SEG_LEN * (seg + 1), :] = weigh(chunk, seg)

    def block_state(chunk):
        total_state = seg_state(xw_buf[:SEG_LEN, :], 0)
        for seg in range(1, segs):
            total_state = (decay_buf[chunk, seg:seg + 1] * total_state
                           + seg_state(xw_buf[SEG_LEN * seg:SEG_LEN * (seg + 1), :], seg))
        s_buf[chunk] = total_state

    def relay(step):
        chunk = step - 3 - delay

        @pl.when((chunk >= 0) & (chunk < chunks))
        def _():
            @pl.when(me > 0)
            def _():
                state_copy(chunk).wait_recv()

            @pl.when(me < seq_devs - 1)
            def _():
                decay = decay_buf[chunk, segs:segs + 1]
                s_buf[chunk] = decay * h_buf[chunk] + s_buf[chunk]

    def forward(step):
        chunk = step - 3 - delay

        @pl.when((chunk >= 0) & (chunk < chunks) & (me < seq_devs - 1))
        def _():
            state_copy(chunk).start()

    def project(step, target, chunk):
        slot = step % 2 if isinstance(step, int) else lax.rem(step, 2)
        target[:, columns_of(chunk)] = jnp.dot(
            out_ref[...], win_buf[slot], preferred_element_type=f32).astype(bf16)

    def ssd_seg(chunk, seg, state_now, gated):
        columns = columns_of(chunk)
        table = decay_buf.at[chunk]
        low = low_half(SEG_LEN)
        rows = slice(SEG_LEN * seg, SEG_LEN * (seg + 1))
        y_state = jnp.dot(c_buf[rows, :], state_now.astype(bf16), preferred_element_type=f32)
        rolled = chunk_heads(log_buf[rows, :], chunk)
        first_head = heads_chunk * chunk
        if not isinstance(chunk, int):
            first_head = pl.multiple_of(first_head, heads_chunk)
        q_rows = q_buf[pl.ds(first_head, heads_chunk), rows]
        x_seg = xs_buf[rows, columns]
        z_seg = z_buf[rows, columns]
        scores = cb_buf[rows, :]
        causal = row_i >= col_i
        for pair in range(heads_chunk // 2):
            lanes = slice(LANES * pair, LANES * (pair + 1))
            logs_pair, mats = [], []
            for head in (2 * pair, 2 * pair + 1):
                log_t = jnp.broadcast_to(rolled[:, head:head + 1], (SEG_LEN, SEG_LEN))
                expo = jnp.where(causal, log_t - q_rows[head:head + 1, :], MASKED)
                mats.append((scores * jnp.exp2(expo)).astype(bf16))
                logs_pair.append(log_t)
            x_pair = x_seg[:, lanes]
            nil = jnp.zeros_like(x_pair)
            rhs = jnp.concatenate([jnp.where(low, x_pair, nil), jnp.where(low, nil, x_pair)], axis=0)
            y_pair = jnp.dot(jnp.concatenate(mats, axis=1), rhs, preferred_element_type=f32)
            y_pair = y_pair + y_state[:, lanes] * jnp.exp2(jnp.where(low, logs_pair[0], logs_pair[1]))
            y_pair = y_pair + table[segs + 1:segs + 2, lanes] * x_pair.astype(f32)
            z_pair = z_seg[:, lanes].astype(f32)
            gated[rows, lanes] = (y_pair * (z_pair / (1.0 + jnp.exp2(z_pair * -LOG2E)))).astype(bf16)
        if seg < segs - 1:
            state_now = table[seg:seg + 1] * state_now + seg_state(weigh(chunk, seg), seg)
        return state_now

    def mix_and_add(chunk, gated, piece_of):
        state_now = h_buf[chunk]
        for seg in range(segs):
            piece_of(seg)
            state_now = ssd_seg(chunk, seg, state_now, gated)

    pl.semaphore_wait(barrier, 2)

    def xs_step(step, carry):
        relay(step)
        win_copy(step).wait()
        win_copy(step + 1).start()
        forward(step)
        weigh_block(step - 2)
        project(step, xs_buf, step - 1)
        block_state(step - 2)
        return carry

    lax.fori_loop(2, chunks + 1, xs_step, 0)

    def z_part(step, chunk):
        cleared = d_model // chunks
        start = cleared * chunk if isinstance(chunk, int) else pl.multiple_of(cleared * chunk, cleared)
        acc[:, pl.ds(start, cleared)] = jnp.zeros((tokens, cleared), f32)
        project(step, z_buf, chunk)

    def z_enter(step):
        step = jnp.int32(step)
        relay(step)
        win_copy(step).wait()
        win_copy(step + 1).start()
        forward(step)

    z_enter(chunks + 1)
    weigh_block(chunks - 1)
    z_part(chunks + 1, 0)
    block_state(chunks - 1)
    wout_copy(jnp.int32(0)).start()

    def z_step(step, carry):
        z_enter(step)
        z_part(step, step - 1 - chunks)
        return carry

    lax.fori_loop(chunks + 2, 2 * chunks, z_step, 0)
    last_z = jnp.int32(2 * chunks)
    relay(last_z)
    win_copy(last_z).wait()
    forward(last_z)
    cleared = d_model // chunks
    acc[:, cleared * (chunks - 1):] = jnp.zeros((tokens, cleared), f32)

    def z_piece(seg):
        if seg % 2 == 0:
            width = 2 * CHUNK // segs
            start = width * (seg // 2)
            z_buf[:, inner - CHUNK + start:inner - CHUNK + start + width] = jnp.dot(
                out_ref[...], win_buf[(2 * chunks) % 2, :, start:start + width], preferred_element_type=f32).astype(bf16)

    mix_and_add(0, gated_a, z_piece)

    def out_part(chunk, gated, piece):
        width = d_model // segs
        cols = slice(width * piece, width * (piece + 1))
        slot = chunk % 2 if isinstance(chunk, int) else lax.rem(chunk, 2)
        acc[:, cols] += jnp.dot(gated[...], wout_buf[slot, :, cols], preferred_element_type=f32)

    def out_enter(chunk):
        chunk = jnp.int32(chunk)
        step = 2 * chunks + chunk
        relay(step)
        wout_copy(chunk - 1).wait()
        wout_copy(chunk).start()
        forward(step)

    def out_chunk(chunk, gated, before):
        out_enter(chunk)
        mix_and_add(chunk, gated, lambda seg: out_part(chunk - 1, before, seg))

    def out_step(pair, carry):
        out_chunk(2 * pair + 1, gated_b, gated_a)
        out_chunk(2 * pair + 2, gated_a, gated_b)
        return carry

    lax.fori_loop(0, chunks // 2 - 1, out_step, 0)
    out_chunk(chunks - 1, gated_b, gated_a)
    final = jnp.int32(chunks - 1)
    wout_copy(final).wait()

    width = d_model // segs
    for piece in range(segs):
        cols = slice(width * piece, width * (piece + 1))
        product = jnp.dot(gated_b[...], wout_buf[(chunks - 1) % 2, :, cols], preferred_element_type=f32)
        out_ref[:, cols] = (out_ref[:, cols].astype(f32) + (acc[:, cols] + product)).astype(bf16)

    @pl.when(me < seq_devs - 1)
    def _():
        def drain(chunk, carry):
            state_copy(chunk).wait_send()
            return carry
        lax.fori_loop(0, chunks, drain, 0)


def solution(mesh):
    seq_devs = mesh.shape["sp"]
    row_spec = P(("dp", "sp"), None)

    def local_mixer(x_loc, w_in, a_neg, dt_bias, d_skip, w_out):
        f32, bf16 = jnp.float32, jnp.bfloat16
        tokens, d_model = x_loc.shape
        inner = w_out.shape[0]
        heads = a_neg.shape[0]
        state = (w_in.shape[1] - 2 * inner - heads) // 2
        chunks = inner // CHUNK
        any_spec = pl.BlockSpec(memory_space=pl.ANY)
        vmem_spec = pl.BlockSpec(memory_space=pltpu.VMEM)
        return pl.pallas_call(
            functools.partial(mixer_kernel, seq_devs),
            out_shape=pltpu.VMEM((tokens, d_model), bf16),
            in_specs=[any_spec, any_spec, vmem_spec, vmem_spec, vmem_spec, any_spec],
            out_specs=vmem_spec,
            scratch_shapes=[
                pltpu.VMEM((2, d_model, CHUNK), bf16),
                pltpu.VMEM((2, CHUNK, d_model), bf16),
                pltpu.VMEM((tokens, inner), bf16),
                pltpu.VMEM((tokens, inner), bf16),
                pltpu.VMEM((tokens, d_model), f32),
                pltpu.VMEM((chunks, state, CHUNK), f32),
                pltpu.VMEM((chunks, state, CHUNK), f32),
                pltpu.VMEM((tokens, CHUNK), bf16),
                pltpu.VMEM((tokens, CHUNK), bf16),
                pltpu.VMEM((tokens, CHUNK), bf16),
                pltpu.VMEM((tokens, state), bf16),
                pltpu.VMEM((state, tokens), bf16),
                pltpu.VMEM((tokens, SEG_LEN), f32),
                pltpu.VMEM((tokens, heads), f32),
                pltpu.VMEM((heads, tokens), f32),
                pltpu.VMEM((tokens, heads), f32),
                pltpu.VMEM((8, heads), f32),
                pltpu.VMEM((chunks, 8, CHUNK), f32),
                pltpu.SemaphoreType.DMA((PIECES,)),
                pltpu.SemaphoreType.DMA((PIECES,)),
                pltpu.SemaphoreType.DMA((PIECES,)),
                pltpu.SemaphoreType.DMA((2,)),
                pltpu.SemaphoreType.DMA((2,)),
                pltpu.SemaphoreType.DMA((chunks,)),
                pltpu.SemaphoreType.DMA((chunks,)),
            ],
            compiler_params=pltpu.CompilerParams(
                collective_id=0, has_side_effects=True, vmem_limit_bytes=62849024),
        )(x_loc, w_in, a_neg[None], dt_bias[None], d_skip[None], w_out)

    return jax.shard_map(local_mixer, mesh=mesh, in_specs=(row_spec, P(), P(), P(), P(), P()),
                         out_specs=row_spec, check_vma=False)
```

```python
import functools

import jax
import jax.numpy as jnp
from jax import lax
from jax.experimental import pallas as pl
from jax.experimental.pallas import tpu as pltpu
from jax.sharding import PartitionSpec as P

SEG_LEN = 128
LANES = 128
CHUNK = 512
PIECES = 4
MASKED = -1e30
LOG2E = 1.4426950408889634


def mixer_kernel(seq_devs, x_hbm, w_in, a_neg, dt_bias, d_skip, w_out, out_ref,
                 win_buf, wout_buf, xs_buf, z_buf, acc, s_buf, h_buf, gated_a, gated_b,
                 xw_buf, c_buf, bt_buf, cb_buf, log_buf, q_buf, w1_buf, row_buf, decay_buf,
                 x_sem, small_sem, first_sem, win_sem, wout_sem, send_sem, recv_sem):
    f32, bf16 = jnp.float32, jnp.bfloat16
    tokens, d_model = out_ref.shape
    inner = xs_buf.shape[1]
    heads = a_neg.shape[1]
    head_dim = inner // heads
    state = c_buf.shape[1]
    chunks = inner // CHUNK
    segs = tokens // SEG_LEN
    heads_chunk = CHUNK // head_dim
    small = 2 * state + heads
    k_tile = d_model // PIECES
    me = lax.axis_index("sp")
    right = lax.rem(me + 1, seq_devs)
    left = lax.rem(me + seq_devs - 1, seq_devs)
    delay = (26 * (me // 2)) // 7 + lax.rem(me, 2)

    barrier = pltpu.get_barrier_semaphore()
    for peer in (left, right):
        pl.semaphore_signal(barrier, inc=1, device_id={"sp": peer}, device_id_type=pl.DeviceIdType.MESH)

    def x_copy(piece):
        cols = pl.ds(k_tile * piece, k_tile)
        return pltpu.make_async_copy(x_hbm.at[:, cols], out_ref.at[:, cols], x_sem.at[piece])

    def small_copy(piece):
        rows = pl.ds(k_tile * piece, k_tile)
        return pltpu.make_async_copy(
            w_in.at[rows, pl.ds(2 * inner, small)], win_buf.at[0, rows, pl.ds(0, small)], small_sem.at[piece])

    def first_copy(piece):
        rows = pl.ds(k_tile * piece, k_tile)
        return pltpu.make_async_copy(
            w_in.at[rows, pl.ds(inner, CHUNK)], win_buf.at[1, rows, :], first_sem.at[piece])

    def win_copy(step):
        column = jnp.where(step <= chunks, inner + CHUNK * (step - 1), CHUNK * (step - 1 - chunks))
        column = pl.multiple_of(column, CHUNK)
        slot = lax.rem(step, 2)
        return pltpu.make_async_copy(w_in.at[:, pl.ds(column, CHUNK)], win_buf.at[slot], win_sem.at[slot])

    def wout_copy(chunk):
        slot = lax.rem(chunk, 2)
        row = pl.multiple_of(CHUNK * chunk, CHUNK)
        return pltpu.make_async_copy(w_out.at[pl.ds(row, CHUNK), :], wout_buf.at[slot], wout_sem.at[slot])

    def state_copy(chunk):
        return pltpu.make_async_remote_copy(
            src_ref=s_buf.at[chunk], dst_ref=h_buf.at[chunk], send_sem=send_sem.at[chunk], recv_sem=recv_sem.at[chunk],
            device_id={"sp": right}, device_id_type=pl.DeviceIdType.MESH)

    for piece in range(PIECES):
        x_copy(piece).start()
        small_copy(piece).start()
    for piece in range(PIECES):
        first_copy(piece).start()

    @pl.when(me == 0)
    def _():
        def clear(chunk, carry):
            h_buf[chunk] = jnp.zeros(h_buf.shape[1:], f32)
            return carry
        lax.fori_loop(0, chunks, clear, 0)

    proj = jnp.zeros((tokens, small), f32)
    for piece in range(PIECES):
        x_copy(piece).wait()
        small_copy(piece).wait()
        part = slice(k_tile * piece, k_tile * (piece + 1))
        proj = proj + jnp.dot(out_ref[:, part], win_buf[0, part, :small], preferred_element_type=f32)
    proj = proj.astype(bf16)
    win_copy(jnp.int32(2)).start()
    for piece in range(PIECES):
        first_copy(piece).wait()
    head, tail = slice(0, d_model // 2), slice(d_model // 2, d_model)
    first = jnp.dot(out_ref[:, head], win_buf[1, head, :], preferred_element_type=f32)
    c_buf[...] = proj[:, state:2 * state]
    bt_buf[...] = proj[:, :state].astype(f32).T.astype(bf16)
    dt = jax.nn.softplus(proj[:, 2 * state:].astype(f32) + dt_bias[...])
    logs = dt * a_neg[...]
    log_dt = jnp.log(dt) * LOG2E
    row_i = lax.broadcasted_iota(jnp.int32, (SEG_LEN, SEG_LEN), 0)
    col_i = lax.broadcasted_iota(jnp.int32, (SEG_LEN, SEG_LEN), 1)
    tri = jnp.where(row_i >= col_i, 1.0, 0.0).astype(f32)
    total = jnp.zeros((1, heads), f32)
    for seg in range(segs):
        rows = slice(SEG_LEN * seg, SEG_LEN * (seg + 1))
        cum = jnp.dot(tri, logs[rows], preferred_element_type=f32, precision=lax.Precision.HIGHEST)
        last = cum[SEG_LEN - 1:]
        log_buf[rows, :] = cum * LOG2E
        q_buf[:, rows] = (cum * LOG2E - log_dt[rows]).T
        w1_buf[rows, :] = jnp.exp(last - cum) * dt[rows]
        row_buf[seg:seg + 1, :] = jnp.exp(last)
        total = total + last
        cb_buf[rows, :] = jnp.dot(c_buf[rows, :], bt_buf[:, rows], preferred_element_type=f32)
    row_buf[segs:segs + 1, :] = jnp.exp(total)
    row_buf[segs + 1:segs + 2, :] = d_skip[...]
    row_buf[segs + 2:8, :] = jnp.zeros((8 - segs - 2, heads), f32)
    first = first + jnp.dot(out_ref[:, tail], win_buf[1, tail, :], preferred_element_type=f32)
    xs_buf[:, :CHUNK] = first.astype(bf16)

    def low_half(rows):
        return lax.broadcasted_iota(jnp.int32, (rows, LANES), 1) < head_dim

    def chunk_heads(values, chunk):
        chunk = jnp.int32(chunk)
        return pltpu.roll(values, lax.rem(heads - heads_chunk * chunk, heads), 1)

    def spread(rolled, pair):
        rows = rolled.shape[0]
        one = jnp.broadcast_to(rolled[:, 2 * pair:2 * pair + 1], (rows, LANES))
        two = jnp.broadcast_to(rolled[:, 2 * pair + 1:2 * pair + 2], (rows, LANES))
        return jnp.where(low_half(rows), one, two)

    def spread_rows(chunk):
        rolled = chunk_heads(row_buf[...], chunk)
        return jnp.concatenate([spread(rolled, pair) for pair in range(heads_chunk // 2)], axis=1)

    def columns_of(chunk):
        if isinstance(chunk, int):
            return slice(CHUNK * chunk, CHUNK * (chunk + 1))
        return pl.ds(pl.multiple_of(CHUNK * chunk, CHUNK), CHUNK)

    def weigh(chunk, seg):
        rows = slice(SEG_LEN * seg, SEG_LEN * (seg + 1))
        rolled = chunk_heads(w1_buf[rows, :], chunk)
        factor = jnp.concatenate([spread(rolled, pair) for pair in range(heads_chunk // 2)], axis=1)
        return (xs_buf[rows, columns_of(chunk)].astype(f32) * factor).astype(bf16)

    def seg_state(weighted, seg):
        return jnp.dot(bt_buf[:, SEG_LEN * seg:SEG_LEN * (seg + 1)], weighted, preferred_element_type=f32)

    def weigh_block(chunk):
        decay_buf[chunk] = spread_rows(chunk)
        for seg in range(segs):
            xw_buf[SEG_LEN * seg:SEG_LEN * (seg + 1), :] = weigh(chunk, seg)

    def block_state(chunk):
        total_state = seg_state(xw_buf[:SEG_LEN, :], 0)
        for seg in range(1, segs):
            total_state = (decay_buf[chunk, seg:seg + 1] * total_state
                           + seg_state(xw_buf[SEG_LEN * seg:SEG_LEN * (seg + 1), :], seg))
        s_buf[chunk] = total_state

    def relayed(step):
        turn = step - 3 - delay
        chunk = turn - turn // 7
        return chunk, (turn >= 0) & (lax.rem(turn, 7) != 6) & (chunk < chunks)

    def relay(step):
        chunk, active = relayed(step)

        @pl.when(active)
        def _():
            @pl.when(me > 0)
            def _():
                state_copy(chunk).wait_recv()

            @pl.when(me < seq_devs - 1)
            def _():
                decay = decay_buf[chunk, segs:segs + 1]
                s_buf[chunk] = decay * h_buf[chunk] + s_buf[chunk]

    def forward(step):
        chunk, active = relayed(step)

        @pl.when(active & (me < seq_devs - 1))
        def _():
            state_copy(chunk).start()

    def project(step, target, chunk):
        slot = step % 2 if isinstance(step, int) else lax.rem(step, 2)
        target[:, columns_of(chunk)] = jnp.dot(
            out_ref[...], win_buf[slot], preferred_element_type=f32).astype(bf16)

    def ssd_seg(chunk, seg, state_now, gated, middle):
        columns = columns_of(chunk)
        table = decay_buf.at[chunk]
        low = low_half(SEG_LEN)
        rows = slice(SEG_LEN * seg, SEG_LEN * (seg + 1))
        y_state = jnp.dot(c_buf[rows, :], state_now.astype(bf16), preferred_element_type=f32)
        rolled = chunk_heads(log_buf[rows, :], chunk)
        first_head = heads_chunk * chunk
        if not isinstance(chunk, int):
            first_head = pl.multiple_of(first_head, heads_chunk)
        q_rows = q_buf[pl.ds(first_head, heads_chunk), rows]
        x_seg = xs_buf[rows, columns]
        z_seg = z_buf[rows, columns]
        scores = cb_buf[rows, :]
        causal = row_i >= col_i
        for pair in range(heads_chunk // 2):
            if pair == heads_chunk // 4:
                middle()
            lanes = slice(LANES * pair, LANES * (pair + 1))
            logs_pair, mats = [], []
            for head in (2 * pair, 2 * pair + 1):
                log_t = jnp.broadcast_to(rolled[:, head:head + 1], (SEG_LEN, SEG_LEN))
                expo = jnp.where(causal, log_t - q_rows[head:head + 1, :], MASKED)
                mats.append((scores * jnp.exp2(expo)).astype(bf16))
                logs_pair.append(log_t)
            x_pair = x_seg[:, lanes]
            nil = jnp.zeros_like(x_pair)
            rhs = jnp.concatenate([jnp.where(low, x_pair, nil), jnp.where(low, nil, x_pair)], axis=0)
            y_pair = jnp.dot(jnp.concatenate(mats, axis=1), rhs, preferred_element_type=f32)
            y_pair = y_pair + y_state[:, lanes] * jnp.exp2(jnp.where(low, logs_pair[0], logs_pair[1]))
            y_pair = y_pair + table[segs + 1:segs + 2, lanes] * x_pair.astype(f32)
            z_pair = z_seg[:, lanes].astype(f32)
            gated[rows, lanes] = (y_pair * (z_pair / (1.0 + jnp.exp2(z_pair * -LOG2E)))).astype(bf16)
        if seg < segs - 1:
            state_now = table[seg:seg + 1] * state_now + seg_state(weigh(chunk, seg), seg)
        return state_now

    def mix_and_add(chunk, gated, piece_of):
        state_now = h_buf[chunk]
        for seg in range(segs):
            piece_of(2 * seg)
            state_now = ssd_seg(chunk, seg, state_now, gated, lambda: piece_of(2 * seg + 1))

    pl.semaphore_wait(barrier, 2)

    def xs_step(step, carry):
        relay(step)
        win_copy(step).wait()
        win_copy(step + 1).start()
        forward(step)
        weigh_block(step - 2)
        project(step, xs_buf, step - 1)
        block_state(step - 2)
        return carry

    lax.fori_loop(2, chunks + 1, xs_step, 0)

    def z_part(step, chunk):
        cleared = d_model // chunks
        start = cleared * chunk if isinstance(chunk, int) else pl.multiple_of(cleared * chunk, cleared)
        acc[:, pl.ds(start, cleared)] = jnp.zeros((tokens, cleared), f32)
        project(step, z_buf, chunk)

    def z_enter(step):
        step = jnp.int32(step)
        relay(step)
        win_copy(step).wait()
        win_copy(step + 1).start()
        forward(step)

    z_enter(chunks + 1)
    weigh_block(chunks - 1)
    z_part(chunks + 1, 0)
    block_state(chunks - 1)
    wout_copy(jnp.int32(0)).start()

    def z_step(step, carry):
        z_enter(step)
        z_part(step, step - 1 - chunks)
        return carry

    lax.fori_loop(chunks + 2, 2 * chunks, z_step, 0)
    last_z = jnp.int32(2 * chunks)
    relay(last_z)
    win_copy(last_z).wait()
    forward(last_z)
    cleared = d_model // chunks
    acc[:, cleared * (chunks - 1):] = jnp.zeros((tokens, cleared), f32)

    def z_piece(seg):
        if seg % segs == 0:
            width = 2 * CHUNK // segs
            start = width * (seg // segs)
            z_buf[:, inner - CHUNK + start:inner - CHUNK + start + width] = jnp.dot(
                out_ref[...], win_buf[(2 * chunks) % 2, :, start:start + width], preferred_element_type=f32).astype(bf16)

    mix_and_add(0, gated_a, z_piece)

    def out_part(chunk, gated, piece):
        width = d_model // (2 * segs)
        cols = slice(width * piece, width * (piece + 1))
        slot = chunk % 2 if isinstance(chunk, int) else lax.rem(chunk, 2)
        acc[:, cols] += jnp.dot(gated[...], wout_buf[slot, :, cols], preferred_element_type=f32)

    def out_enter(chunk):
        chunk = jnp.int32(chunk)
        step = 2 * chunks + chunk
        relay(step)
        wout_copy(chunk - 1).wait()
        wout_copy(chunk).start()
        forward(step)

    def out_chunk(chunk, gated, before):
        out_enter(chunk)
        mix_and_add(chunk, gated, lambda seg: out_part(chunk - 1, before, seg))

    def out_step(pair, carry):
        out_chunk(2 * pair + 1, gated_b, gated_a)
        out_chunk(2 * pair + 2, gated_a, gated_b)
        return carry

    lax.fori_loop(0, chunks // 2 - 1, out_step, 0)
    out_chunk(chunks - 1, gated_b, gated_a)
    final = jnp.int32(chunks - 1)
    wout_copy(final).wait()

    width = d_model // segs
    for piece in range(segs):
        cols = slice(width * piece, width * (piece + 1))
        product = jnp.dot(gated_b[...], wout_buf[(chunks - 1) % 2, :, cols], preferred_element_type=f32)
        out_ref[:, cols] = (out_ref[:, cols].astype(f32) + (acc[:, cols] + product)).astype(bf16)

    @pl.when(me < seq_devs - 1)
    def _():
        def drain(chunk, carry):
            state_copy(chunk).wait_send()
            return carry
        lax.fori_loop(0, chunks, drain, 0)


def solution(mesh):
    seq_devs = mesh.shape["sp"]
    row_spec = P(("dp", "sp"), None)

    def local_mixer(x_loc, w_in, a_neg, dt_bias, d_skip, w_out):
        f32, bf16 = jnp.float32, jnp.bfloat16
        tokens, d_model = x_loc.shape
        inner = w_out.shape[0]
        heads = a_neg.shape[0]
        state = (w_in.shape[1] - 2 * inner - heads) // 2
        chunks = inner // CHUNK
        any_spec = pl.BlockSpec(memory_space=pl.ANY)
        vmem_spec = pl.BlockSpec(memory_space=pltpu.VMEM)
        return pl.pallas_call(
            functools.partial(mixer_kernel, seq_devs),
            out_shape=pltpu.VMEM((tokens, d_model), bf16),
            in_specs=[any_spec, any_spec, vmem_spec, vmem_spec, vmem_spec, any_spec],
            out_specs=vmem_spec,
            scratch_shapes=[
                pltpu.VMEM((2, d_model, CHUNK), bf16),
                pltpu.VMEM((2, CHUNK, d_model), bf16),
                pltpu.VMEM((tokens, inner), bf16),
                pltpu.VMEM((tokens, inner), bf16),
                pltpu.VMEM((tokens, d_model), f32),
                pltpu.VMEM((chunks, state, CHUNK), f32),
                pltpu.VMEM((chunks, state, CHUNK), f32),
                pltpu.VMEM((tokens, CHUNK), bf16),
                pltpu.VMEM((tokens, CHUNK), bf16),
                pltpu.VMEM((tokens, CHUNK), bf16),
                pltpu.VMEM((tokens, state), bf16),
                pltpu.VMEM((state, tokens), bf16),
                pltpu.VMEM((tokens, SEG_LEN), f32),
                pltpu.VMEM((tokens, heads), f32),
                pltpu.VMEM((heads, tokens), f32),
                pltpu.VMEM((tokens, heads), f32),
                pltpu.VMEM((8, heads), f32),
                pltpu.VMEM((chunks, 8, CHUNK), f32),
                pltpu.SemaphoreType.DMA((PIECES,)),
                pltpu.SemaphoreType.DMA((PIECES,)),
                pltpu.SemaphoreType.DMA((PIECES,)),
                pltpu.SemaphoreType.DMA((2,)),
                pltpu.SemaphoreType.DMA((2,)),
                pltpu.SemaphoreType.DMA((chunks,)),
                pltpu.SemaphoreType.DMA((chunks,)),
            ],
            compiler_params=pltpu.CompilerParams(
                collective_id=0, has_side_effects=True, vmem_limit_bytes=62849024),
        )(x_loc, w_in, a_neg[None], dt_bias[None], d_skip[None], w_out)

    return jax.shard_map(local_mixer, mesh=mesh, in_specs=(row_spec, P(), P(), P(), P(), P()),
                         out_specs=row_spec, check_vma=False)
```

```python
import functools

import jax
import jax.numpy as jnp
from jax import lax
from jax.experimental import pallas as pl
from jax.experimental.pallas import tpu as pltpu
from jax.sharding import PartitionSpec as P

SEG_LEN = 128
LANES = 128
CHUNK = 512
PIECES = 4
MASKED = -1e30
LOG2E = 1.4426950408889634


def mixer_kernel(seq_devs, x_hbm, w_in, a_neg, dt_bias, d_skip, w_out, out_ref,
                 win_buf, wout_buf, xs_buf, z_buf, acc, s_buf, h_buf, gated_a, gated_b,
                 xw_buf, c_buf, bt_buf, cb_buf, log_buf, q_buf, w1_buf, row_buf, decay_buf,
                 x_sem, small_sem, first_sem, win_sem, wout_sem, send_sem, recv_sem):
    f32, bf16 = jnp.float32, jnp.bfloat16
    tokens, d_model = out_ref.shape
    inner = xs_buf.shape[1]
    heads = a_neg.shape[1]
    head_dim = inner // heads
    state = c_buf.shape[1]
    chunks = inner // CHUNK
    segs = tokens // SEG_LEN
    heads_chunk = CHUNK // head_dim
    small = 2 * state + heads
    k_tile = d_model // PIECES
    me = lax.axis_index("sp")
    right = lax.rem(me + 1, seq_devs)
    left = lax.rem(me + seq_devs - 1, seq_devs)
    chip = me // 2
    later = (chip + 7) // 8
    delay = (7 * chip + 3 * later) // 2 + lax.rem(me, 2) * (3 - 2 * later)

    barrier = pltpu.get_barrier_semaphore()
    for peer in (left, right):
        pl.semaphore_signal(barrier, inc=1, device_id={"sp": peer}, device_id_type=pl.DeviceIdType.MESH)

    def x_copy(piece):
        cols = pl.ds(k_tile * piece, k_tile)
        return pltpu.make_async_copy(x_hbm.at[:, cols], out_ref.at[:, cols], x_sem.at[piece])

    def small_copy(piece):
        rows = pl.ds(k_tile * piece, k_tile)
        return pltpu.make_async_copy(
            w_in.at[rows, pl.ds(2 * inner, small)], win_buf.at[0, rows, pl.ds(0, small)], small_sem.at[piece])

    def first_copy(piece):
        rows = pl.ds(k_tile * piece, k_tile)
        return pltpu.make_async_copy(
            w_in.at[rows, pl.ds(inner, CHUNK)], win_buf.at[1, rows, :], first_sem.at[piece])

    def win_copy(step):
        column = jnp.where(step <= chunks, inner + CHUNK * (step - 1), CHUNK * (step - 1 - chunks))
        column = pl.multiple_of(column, CHUNK)
        slot = lax.rem(step, 2)
        return pltpu.make_async_copy(w_in.at[:, pl.ds(column, CHUNK)], win_buf.at[slot], win_sem.at[slot])

    def wout_copy(chunk):
        slot = lax.rem(chunk, 2)
        row = pl.multiple_of(CHUNK * chunk, CHUNK)
        return pltpu.make_async_copy(w_out.at[pl.ds(row, CHUNK), :], wout_buf.at[slot], wout_sem.at[slot])

    def state_copy(chunk):
        return pltpu.make_async_remote_copy(
            src_ref=s_buf.at[chunk], dst_ref=h_buf.at[chunk], send_sem=send_sem.at[chunk], recv_sem=recv_sem.at[chunk],
            device_id={"sp": right}, device_id_type=pl.DeviceIdType.MESH)

    for piece in range(PIECES):
        x_copy(piece).start()
        small_copy(piece).start()
    for piece in range(PIECES):
        first_copy(piece).start()

    @pl.when(me == 0)
    def _():
        def clear(chunk, carry):
            h_buf[chunk] = jnp.zeros(h_buf.shape[1:], f32)
            return carry
        lax.fori_loop(0, chunks, clear, 0)

    proj = jnp.zeros((tokens, small), f32)
    for piece in range(PIECES):
        x_copy(piece).wait()
        small_copy(piece).wait()
        part = slice(k_tile * piece, k_tile * (piece + 1))
        proj = proj + jnp.dot(out_ref[:, part], win_buf[0, part, :small], preferred_element_type=f32)
    proj = proj.astype(bf16)
    win_copy(jnp.int32(2)).start()
    for piece in range(PIECES):
        first_copy(piece).wait()
    head, tail = slice(0, d_model // 2), slice(d_model // 2, d_model)
    first = jnp.dot(out_ref[:, head], win_buf[1, head, :], preferred_element_type=f32)
    c_buf[...] = proj[:, state:2 * state]
    bt_buf[...] = proj[:, :state].astype(f32).T.astype(bf16)
    dt = jax.nn.softplus(proj[:, 2 * state:].astype(f32) + dt_bias[...])
    logs = dt * a_neg[...]
    log_dt = jnp.log(dt) * LOG2E
    row_i = lax.broadcasted_iota(jnp.int32, (SEG_LEN, SEG_LEN), 0)
    col_i = lax.broadcasted_iota(jnp.int32, (SEG_LEN, SEG_LEN), 1)
    tri = jnp.where(row_i >= col_i, 1.0, 0.0).astype(f32)
    total = jnp.zeros((1, heads), f32)
    for seg in range(segs):
        rows = slice(SEG_LEN * seg, SEG_LEN * (seg + 1))
        cum = jnp.dot(tri, logs[rows], preferred_element_type=f32, precision=lax.Precision.HIGHEST)
        last = cum[SEG_LEN - 1:]
        log_buf[rows, :] = cum * LOG2E
        q_buf[:, rows] = (cum * LOG2E - log_dt[rows]).T
        w1_buf[rows, :] = jnp.exp(last - cum) * dt[rows]
        row_buf[seg:seg + 1, :] = jnp.exp(last)
        total = total + last
        cb_buf[rows, :] = jnp.dot(c_buf[rows, :], bt_buf[:, rows], preferred_element_type=f32)
    row_buf[segs:segs + 1, :] = jnp.exp(total)
    row_buf[segs + 1:segs + 2, :] = d_skip[...]
    row_buf[segs + 2:8, :] = jnp.zeros((8 - segs - 2, heads), f32)
    first = first + jnp.dot(out_ref[:, tail], win_buf[1, tail, :], preferred_element_type=f32)
    xs_buf[:, :CHUNK] = first.astype(bf16)

    def low_half(rows):
        return lax.broadcasted_iota(jnp.int32, (rows, LANES), 1) < head_dim

    def chunk_heads(values, chunk):
        chunk = jnp.int32(chunk)
        return pltpu.roll(values, lax.rem(heads - heads_chunk * chunk, heads), 1)

    def spread(rolled, pair):
        rows = rolled.shape[0]
        one = jnp.broadcast_to(rolled[:, 2 * pair:2 * pair + 1], (rows, LANES))
        two = jnp.broadcast_to(rolled[:, 2 * pair + 1:2 * pair + 2], (rows, LANES))
        return jnp.where(low_half(rows), one, two)

    def spread_rows(chunk):
        rolled = chunk_heads(row_buf[...], chunk)
        return jnp.concatenate([spread(rolled, pair) for pair in range(heads_chunk // 2)], axis=1)

    def columns_of(chunk):
        if isinstance(chunk, int):
            return slice(CHUNK * chunk, CHUNK * (chunk + 1))
        return pl.ds(pl.multiple_of(CHUNK * chunk, CHUNK), CHUNK)

    def weigh(chunk, seg):
        rows = slice(SEG_LEN * seg, SEG_LEN * (seg + 1))
        rolled = chunk_heads(w1_buf[rows, :], chunk)
        factor = jnp.concatenate([spread(rolled, pair) for pair in range(heads_chunk // 2)], axis=1)
        return (xs_buf[rows, columns_of(chunk)].astype(f32) * factor).astype(bf16)

    def seg_state(weighted, seg):
        return jnp.dot(bt_buf[:, SEG_LEN * seg:SEG_LEN * (seg + 1)], weighted, preferred_element_type=f32)

    def weigh_block(chunk):
        decay_buf[chunk] = spread_rows(chunk)
        for seg in range(segs):
            xw_buf[SEG_LEN * seg:SEG_LEN * (seg + 1), :] = weigh(chunk, seg)

    def block_state(chunk):
        total_state = seg_state(xw_buf[:SEG_LEN, :], 0)
        for seg in range(1, segs):
            total_state = (decay_buf[chunk, seg:seg + 1] * total_state
                           + seg_state(xw_buf[SEG_LEN * seg:SEG_LEN * (seg + 1), :], seg))
        s_buf[chunk] = total_state

    def relayed(step):
        turn = step - 3 - delay
        chunk = turn - turn // 7
        return chunk, (turn >= 0) & (lax.rem(turn, 7) != 6) & (chunk < chunks)

    def relay(step):
        chunk, active = relayed(step)

        @pl.when(active)
        def _():
            @pl.when(me > 0)
            def _():
                state_copy(chunk).wait_recv()

            @pl.when(me < seq_devs - 1)
            def _():
                decay = decay_buf[chunk, segs:segs + 1]
                s_buf[chunk] = decay * h_buf[chunk] + s_buf[chunk]

    def forward(step):
        chunk, active = relayed(step)

        @pl.when(active & (me < seq_devs - 1))
        def _():
            state_copy(chunk).start()

    def project(step, target, chunk):
        slot = step % 2 if isinstance(step, int) else lax.rem(step, 2)
        target[:, columns_of(chunk)] = jnp.dot(
            out_ref[...], win_buf[slot], preferred_element_type=f32).astype(bf16)

    def ssd_seg(chunk, seg, state_now, gated, middle):
        columns = columns_of(chunk)
        table = decay_buf.at[chunk]
        low = low_half(SEG_LEN)
        rows = slice(SEG_LEN * seg, SEG_LEN * (seg + 1))
        y_state = jnp.dot(c_buf[rows, :], state_now.astype(bf16), preferred_element_type=f32)
        rolled = chunk_heads(log_buf[rows, :], chunk)
        first_head = heads_chunk * chunk
        if not isinstance(chunk, int):
            first_head = pl.multiple_of(first_head, heads_chunk)
        q_rows = q_buf[pl.ds(first_head, heads_chunk), rows]
        x_seg = xs_buf[rows, columns]
        z_seg = z_buf[rows, columns]
        scores = cb_buf[rows, :]
        causal = row_i >= col_i
        for pair in range(heads_chunk // 2):
            if pair == heads_chunk // 4:
                middle()
            lanes = slice(LANES * pair, LANES * (pair + 1))
            logs_pair, mats = [], []
            for head in (2 * pair, 2 * pair + 1):
                log_t = jnp.broadcast_to(rolled[:, head:head + 1], (SEG_LEN, SEG_LEN))
                expo = jnp.where(causal, log_t - q_rows[head:head + 1, :], MASKED)
                mats.append((scores * jnp.exp2(expo)).astype(bf16))
                logs_pair.append(log_t)
            x_pair = x_seg[:, lanes]
            nil = jnp.zeros_like(x_pair)
            rhs = jnp.concatenate([jnp.where(low, x_pair, nil), jnp.where(low, nil, x_pair)], axis=0)
            y_pair = jnp.dot(jnp.concatenate(mats, axis=1), rhs, preferred_element_type=f32)
            y_pair = y_pair + y_state[:, lanes] * jnp.exp2(jnp.where(low, logs_pair[0], logs_pair[1]))
            y_pair = y_pair + table[segs + 1:segs + 2, lanes] * x_pair.astype(f32)
            z_pair = z_seg[:, lanes].astype(f32)
            gated[rows, lanes] = (y_pair * (z_pair / (1.0 + jnp.exp2(z_pair * -LOG2E)))).astype(bf16)
        if seg < segs - 1:
            state_now = table[seg:seg + 1] * state_now + seg_state(weigh(chunk, seg), seg)
        return state_now

    def mix_and_add(chunk, gated, piece_of):
        state_now = h_buf[chunk]
        for seg in range(segs):
            piece_of(2 * seg)
            state_now = ssd_seg(chunk, seg, state_now, gated, lambda: piece_of(2 * seg + 1))

    pl.semaphore_wait(barrier, 2)

    def xs_step(step, carry):
        relay(step)
        win_copy(step).wait()
        win_copy(step + 1).start()
        forward(step)
        weigh_block(step - 2)
        project(step, xs_buf, step - 1)
        block_state(step - 2)
        return carry

    lax.fori_loop(2, chunks + 1, xs_step, 0)

    def z_part(step, chunk):
        cleared = d_model // chunks
        start = cleared * chunk if isinstance(chunk, int) else pl.multiple_of(cleared * chunk, cleared)
        acc[:, pl.ds(start, cleared)] = jnp.zeros((tokens, cleared), f32)
        project(step, z_buf, chunk)

    def z_enter(step):
        step = jnp.int32(step)
        relay(step)
        win_copy(step).wait()
        win_copy(step + 1).start()
        forward(step)

    z_enter(chunks + 1)
    weigh_block(chunks - 1)
    z_part(chunks + 1, 0)
    block_state(chunks - 1)
    wout_copy(jnp.int32(0)).start()

    def z_step(step, carry):
        z_enter(step)
        z_part(step, step - 1 - chunks)
        return carry

    lax.fori_loop(chunks + 2, 2 * chunks, z_step, 0)
    last_z = jnp.int32(2 * chunks)
    relay(last_z)
    win_copy(last_z).wait()
    forward(last_z)
    cleared = d_model // chunks
    acc[:, cleared * (chunks - 1):] = jnp.zeros((tokens, cleared), f32)

    def z_piece(seg):
        if seg % segs == 0:
            width = 2 * CHUNK // segs
            start = width * (seg // segs)
            z_buf[:, inner - CHUNK + start:inner - CHUNK + start + width] = jnp.dot(
                out_ref[...], win_buf[(2 * chunks) % 2, :, start:start + width], preferred_element_type=f32).astype(bf16)

    mix_and_add(0, gated_a, z_piece)

    def out_part(chunk, gated, piece):
        width = d_model // (2 * segs)
        cols = slice(width * piece, width * (piece + 1))
        slot = chunk % 2 if isinstance(chunk, int) else lax.rem(chunk, 2)
        acc[:, cols] += jnp.dot(gated[...], wout_buf[slot, :, cols], preferred_element_type=f32)

    def out_enter(chunk):
        chunk = jnp.int32(chunk)
        step = 2 * chunks + chunk
        relay(step)
        wout_copy(chunk - 1).wait()
        wout_copy(chunk).start()
        forward(step)

    def out_chunk(chunk, gated, before):
        out_enter(chunk)
        mix_and_add(chunk, gated, lambda seg: out_part(chunk - 1, before, seg))

    def out_step(pair, carry):
        out_chunk(2 * pair + 1, gated_b, gated_a)
        out_chunk(2 * pair + 2, gated_a, gated_b)
        return carry

    lax.fori_loop(0, chunks // 2 - 1, out_step, 0)
    out_chunk(chunks - 1, gated_b, gated_a)
    final = jnp.int32(chunks - 1)
    wout_copy(final).wait()

    width = d_model // segs
    for piece in range(segs):
        cols = slice(width * piece, width * (piece + 1))
        product = jnp.dot(gated_b[...], wout_buf[(chunks - 1) % 2, :, cols], preferred_element_type=f32)
        out_ref[:, cols] = (out_ref[:, cols].astype(f32) + (acc[:, cols] + product)).astype(bf16)

    @pl.when(me < seq_devs - 1)
    def _():
        def drain(chunk, carry):
            state_copy(chunk).wait_send()
            return carry
        lax.fori_loop(0, chunks, drain, 0)


def solution(mesh):
    seq_devs = mesh.shape["sp"]
    row_spec = P(("dp", "sp"), None)

    def local_mixer(x_loc, w_in, a_neg, dt_bias, d_skip, w_out):
        f32, bf16 = jnp.float32, jnp.bfloat16
        tokens, d_model = x_loc.shape
        inner = w_out.shape[0]
        heads = a_neg.shape[0]
        state = (w_in.shape[1] - 2 * inner - heads) // 2
        chunks = inner // CHUNK
        any_spec = pl.BlockSpec(memory_space=pl.ANY)
        vmem_spec = pl.BlockSpec(memory_space=pltpu.VMEM)
        return pl.pallas_call(
            functools.partial(mixer_kernel, seq_devs),
            out_shape=pltpu.VMEM((tokens, d_model), bf16),
            in_specs=[any_spec, any_spec, vmem_spec, vmem_spec, vmem_spec, any_spec],
            out_specs=vmem_spec,
            scratch_shapes=[
                pltpu.VMEM((2, d_model, CHUNK), bf16),
                pltpu.VMEM((2, CHUNK, d_model), bf16),
                pltpu.VMEM((tokens, inner), bf16),
                pltpu.VMEM((tokens, inner), bf16),
                pltpu.VMEM((tokens, d_model), f32),
                pltpu.VMEM((chunks, state, CHUNK), f32),
                pltpu.VMEM((chunks, state, CHUNK), f32),
                pltpu.VMEM((tokens, CHUNK), bf16),
                pltpu.VMEM((tokens, CHUNK), bf16),
                pltpu.VMEM((tokens, CHUNK), bf16),
                pltpu.VMEM((tokens, state), bf16),
                pltpu.VMEM((state, tokens), bf16),
                pltpu.VMEM((tokens, SEG_LEN), f32),
                pltpu.VMEM((tokens, heads), f32),
                pltpu.VMEM((heads, tokens), f32),
                pltpu.VMEM((tokens, heads), f32),
                pltpu.VMEM((8, heads), f32),
                pltpu.VMEM((chunks, 8, CHUNK), f32),
                pltpu.SemaphoreType.DMA((PIECES,)),
                pltpu.SemaphoreType.DMA((PIECES,)),
                pltpu.SemaphoreType.DMA((PIECES,)),
                pltpu.SemaphoreType.DMA((2,)),
                pltpu.SemaphoreType.DMA((2,)),
                pltpu.SemaphoreType.DMA((chunks,)),
                pltpu.SemaphoreType.DMA((chunks,)),
            ],
            compiler_params=pltpu.CompilerParams(
                collective_id=0, has_side_effects=True, vmem_limit_bytes=62849024),
        )(x_loc, w_in, a_neg[None], dt_bias[None], d_skip[None], w_out)

    return jax.shard_map(local_mixer, mesh=mesh, in_specs=(row_spec, P(), P(), P(), P(), P()),
                         out_specs=row_spec, check_vma=False)
```
